32 devices in a mesh: dp: 8 (over z, y), seq: 4 (over x, core).
Axes of the slice: x: 2, y: 2, z: 4, core: 2. Of those that a mesh axis runs over, the one named last changes fastest.
Arguments:
- layer_input: bfloat16 [8, 512, 2048], P('dp', 'seq'), may hold values from -6 to 6
- writes_first: bfloat16 [8, 512, 128], P('dp', 'seq'), may hold values from -0.375 to 0.375
- reads_first: bfloat16 [8, 512, 128], P('dp', 'seq'), may hold values from -0.375 to 0.375
- decay_first: float32 [8, 32, 512], P('dp', None, 'seq'), may hold values from -1.5 to 0, as said below
- skip_first: float32 [32], replicated, may hold values from 0.5 to 1.5
- writes_second: bfloat16 [8, 512, 128], P('dp', 'seq'), may hold values from -0.375 to 0.375
- reads_second: bfloat16 [8, 512, 128], P('dp', 'seq'), may hold values from -0.375 to 0.375
- decay_second: float32 [8, 32, 512], P('dp', None, 'seq'), may hold values from -1.5 to 0, as said below
- skip_second: float32 [32], replicated, may hold values from 0.5 to 1.5
- order_first: int32 [512], P('seq'), may hold values from 0 to 511, as said below
- order_second: int32 [512], P('seq'), may hold values from 0 to 511, as said below
- cotangent: float32 [8, 512, 2048], P('dp', 'seq'), may hold values from -48 to 48
Outputs:
- grad_input: bfloat16 [8, 512, 2048], P('dp', 'seq')
- grad_writes_first: bfloat16 [8, 512, 128], P('dp', 'seq')
- grad_reads_first: bfloat16 [8, 512, 128], P('dp', 'seq')
- grad_decay_first: float32 [8, 32, 512], P('dp', None, 'seq')
- grad_skip_first: float32 [32], replicated
- grad_writes_second: bfloat16 [8, 512, 128], P('dp', 'seq')
- grad_reads_second: bfloat16 [8, 512, 128], P('dp', 'seq')
- grad_decay_second: float32 [8, 32, 512], P('dp', None, 'seq')
- grad_skip_second: float32 [32], replicated
The draws below stay inside these ranges and needn't reach their ends.
Inputs may be any that keep to these rules, and one draw needn't show every extreme that they name: order_first lists the cells of a 16 by 32 grid (cell i * 32 + j for row i, column j) row after row from row 0 on, each row left to right or right to left. order_second lists the same cells column after column from column 0 on, each column top to bottom or bottom to top. `decay_first`: every entry is negative. `decay_second`: every entry is negative.
All inputs are finite; a program needn't handle non-finite values.
Results may differ from the reference program's by a relative error of at most 0.005.
Values may be sent and summed in bfloat16 or wider, within the bound.
A program may use at most 128 MiB of HBM per device.

```python
import math
import jax
import jax.numpy as jnp
from jax import lax

HEADS = 32
HEAD_DIM = 64
STATE = 128
GROUP = 128
COLS = 32
WIDTH = 2048
ROWS = 16
CLIP_TOKENS = 512
CLIP_COUNT = 8


def decay_law(key):
    random_key_sequence = jax.random.split(key, 6)
    fast_share = 0.5
    is_fast = jax.random.uniform(random_key_sequence[0], (HEADS,)) < fast_share
    fast_rate = jnp.exp(jax.random.uniform(random_key_sequence[1], (HEADS,), minval=jnp.log(1.0 / 50.0), maxval=jnp.log(1.0 / 30.0)))
    slow_rate = jnp.exp(jax.random.uniform(random_key_sequence[2], (HEADS,), minval=jnp.log(0.05), maxval=jnp.log(0.35))) / CLIP_TOKENS
    base_rate = jnp.where(is_fast, fast_rate, slow_rate)
    roughness = jax.random.uniform(random_key_sequence[3], (CLIP_COUNT, HEADS, CLIP_TOKENS), minval=0.5, maxval=1.5)
    block_scale = jnp.exp(jax.random.uniform(random_key_sequence[4], (CLIP_COUNT, 1, CLIP_TOKENS // GROUP), minval=jnp.log(0.6), maxval=jnp.log(1.6)))
    block_scale = jnp.repeat(block_scale, GROUP, axis=2)
    decay_rate_every = base_rate[None, :, None] * roughness * block_scale
    spike_random_keys = jax.random.split(random_key_sequence[5], 2)
    spike_location = jax.random.randint(spike_random_keys[0], (CLIP_COUNT, 2), 0, CLIP_TOKENS)
    spike_penalty_loss = jax.random.uniform(spike_random_keys[1], (CLIP_COUNT, 2), minval=0.2, maxval=0.5)
    token_position = jnp.arange(CLIP_TOKENS, dtype=jnp.int32)
    spike_penalty_terms = (token_position[None, None, :] == spike_location[:, :, None]).astype(jnp.float32) * jnp.log(1.0 - spike_penalty_loss)[:, :, None]
    return (jnp.sum(spike_penalty_terms, axis=1)[:, None, :] - decay_rate_every).astype(jnp.float32)


def draw_decay_first(key, part):
    return decay_law(jax.random.fold_in(key, 11))


def draw_decay_second(key, part):
    return decay_law(jax.random.fold_in(key, 12))


def draw_order_first(key, part):
    reversed_rows = jax.random.randint(jax.random.fold_in(key, 21), (ROWS,), 0, 2)
    token_position = jnp.arange(CLIP_TOKENS, dtype=jnp.int32)
    row_ids = token_position // COLS
    col_ids = token_position % COLS
    return (row_ids * COLS + jnp.where(reversed_rows[row_ids] == 1, COLS - 1 - col_ids, col_ids)).astype(jnp.int32)


def draw_order_second(key, part):
    reversed_cols = jax.random.randint(jax.random.fold_in(key, 22), (COLS,), 0, 2)
    token_position = jnp.arange(CLIP_TOKENS, dtype=jnp.int32)
    col_ids = token_position // ROWS
    row_ids = token_position % ROWS
    return (jnp.where(reversed_cols[col_ids] == 1, ROWS - 1 - row_ids, row_ids) * COLS + col_ids).astype(jnp.int32)


def draw_cotangent(key, part):
    key_one = jax.random.fold_in(key, 31)
    clip_rise = 3.0 ** (jnp.arange(CLIP_COUNT, dtype=jnp.float32) / CLIP_COUNT)
    token_position = jnp.arange(CLIP_TOKENS, dtype=jnp.float32) / CLIP_TOKENS
    noise_all = jnp.clip(jax.random.normal(key_one, (CLIP_COUNT, CLIP_TOKENS, HEADS * HEAD_DIM)), -5.0, 5.0)
    seq_rise = 3.0 ** token_position
    return (noise_all * clip_rise[:, None, None] * seq_rise[None, :, None]).astype(jnp.float32)


def steps_of(own_key, shape, cuts, least, high):
    gain = 1.0
    for dim, shards_of in cuts:
        draws = jax.random.uniform(jax.random.fold_in(jax.random.fold_in(own_key, 6), dim), (shards_of,), jnp.float32, least / len(cuts), high / len(cuts))
        gain = gain * jnp.repeat(jnp.exp(draws), shape[dim] // shards_of).reshape((-1,) + (1,) * (len(shape) - 1 - dim))
    return gain


def noise(rng, dims, deviation, bound, shards=(), kind=jnp.bfloat16):
    drawn = jax.random.normal(rng, dims, jnp.float32) * deviation
    if len(shards) > 0:
        drawn = steps_of(rng, dims, shards, -0.22, 0.18) * drawn
    return jnp.clip(drawn, min=-bound, max=bound).astype(kind)


def setup_inputs(seed: int = 0) -> dict:
    keys = jax.random.split(jax.random.key(seed), 13)
    return {
        "layer_input": noise(keys[0], (CLIP_COUNT, CLIP_TOKENS, WIDTH), 1.0, 6.0, ((0, 8), (1, 4))),
        "writes_first": noise(keys[1], (CLIP_COUNT, CLIP_TOKENS, STATE), ((CLIP_TOKENS * STATE) ** -0.25), 0.375, ((0, 8), (1, 4))),
        "reads_first": noise(keys[2], (CLIP_COUNT, CLIP_TOKENS, STATE), ((CLIP_TOKENS * STATE) ** -0.25), 0.375, ((0, 8), (1, 4))),
        "decay_first": draw_decay_first(jax.random.fold_in(keys[12], 71), 0),
        "skip_first": jnp.clip(jax.random.uniform(keys[4], (HEADS,), jnp.float32, 0.5, 1.5), 0.5, 1.5),
        "writes_second": noise(keys[5], (CLIP_COUNT, CLIP_TOKENS, STATE), ((CLIP_TOKENS * STATE) ** -0.25), 0.375, ((0, 8), (1, 4))),
        "reads_second": noise(keys[6], (CLIP_COUNT, CLIP_TOKENS, STATE), ((CLIP_TOKENS * STATE) ** -0.25), 0.375, ((0, 8), (1, 4))),
        "decay_second": draw_decay_second(jax.random.fold_in(keys[12], 71), 0),
        "skip_second": jnp.clip(jax.random.uniform(keys[8], (HEADS,), jnp.float32, 0.5, 1.5), 0.5, 1.5),
        "order_first": draw_order_first(jax.random.fold_in(keys[12], 71), 0),
        "order_second": draw_order_second(jax.random.fold_in(keys[12], 71), 0),
        "cotangent": draw_cotangent(jax.random.fold_in(keys[12], 71), 0),
    }


highest = lax.Precision.HIGHEST

def group_step(carried, pieces, skip):
    inputs, writes, reads, log_decay = pieces
    running = jnp.cumsum(log_decay, axis=0)
    length = inputs.shape[0]
    causal = jnp.tril(jnp.ones((length, length), dtype=bool))
    scores = jnp.dot(reads, writes.T, precision=highest)
    log_gap = running.T[:, :, None] - running.T[:, None, :]
    weights = jnp.where(causal[None], jnp.exp(jnp.where(causal[None], log_gap, 0.0)), 0.0) * scores[None]
    outputs = jnp.einsum('hts,shp->thp', weights, inputs, precision=highest)
    carried_out = jnp.einsum('hpn,tn->thp', carried, reads, precision=highest)
    outputs = outputs + jnp.exp(running)[:, :, None] * carried_out + skip[None, :, None] * inputs
    totals = running[-1]
    scaled = inputs * jnp.exp(totals[None, :] - running)[:, :, None]
    carried = jnp.exp(totals)[:, None, None] * carried + jnp.einsum('shp,sn->hpn', scaled, writes, precision=highest)
    return (carried, outputs)

def run_layer(inputs, writes, reads, log_decay, skip, carried):
    length, features = inputs.shape
    head_count = log_decay.shape[1]
    head_size = features // head_count
    block_count = length // GROUP
    stacked = (inputs.reshape(block_count, GROUP, head_count, head_size), writes.reshape(block_count, GROUP, writes.shape[1]), reads.reshape(block_count, GROUP, reads.shape[1]), log_decay.reshape(block_count, GROUP, head_count))
    carried, outputs = lax.scan(lambda carry_now, pieces: group_step(carry_now, pieces, skip), carried, stacked)
    return (outputs.reshape(length, features), carried)

def reference(layer_input, writes_first, reads_first, decay_first, skip_first, writes_second, reads_second, decay_second, skip_second, order_first, order_second, cotangent):
    features = HEADS * HEAD_DIM
    empty_state = jnp.zeros((HEADS, HEAD_DIM, STATE), jnp.float32)

    def layer_pair(inputs, writes_one, reads_one, decay_one, skip_one, writes_two, reads_two, decay_two, skip_two):
        first_out = run_layer(inputs.astype(jnp.float32), writes_one.astype(jnp.float32), reads_one.astype(jnp.float32), decay_one.T, skip_one, empty_state)[0]
        lattice = jnp.zeros((CLIP_TOKENS, features), jnp.bfloat16).at[order_first].set(first_out.astype(jnp.bfloat16))
        second_in = lattice[order_second]
        return run_layer(second_in.astype(jnp.float32), writes_two.astype(jnp.float32), reads_two.astype(jnp.float32), decay_two.T, skip_two, empty_state)[0]

    def per_clip(pieces):
        inputs, writes_one, reads_one, decay_one, writes_two, reads_two, decay_two, upstream = pieces
        _, pullback = jax.vjp(layer_pair, inputs, writes_one, reads_one, decay_one, skip_first, writes_two, reads_two, decay_two, skip_second)
        return pullback(upstream)
    grads = lax.map(per_clip, (layer_input, writes_first, reads_first, decay_first, writes_second, reads_second, decay_second, cotangent))
    factor = 1.0 / math.sqrt(CLIP_COUNT * CLIP_TOKENS * HEAD_DIM)
    return (grads[0], grads[1], grads[2], grads[3], lax.optimization_barrier(jnp.sum(grads[4], axis=0)) * factor, grads[5], grads[6], grads[7], lax.optimization_barrier(jnp.sum(grads[8], axis=0)) * factor)
```

```python
import functools
import math

import jax
import jax.numpy as jnp
from jax import lax
from jax.experimental import pallas as pl
from jax.experimental.pallas import tpu as pltpu
from jax.sharding import PartitionSpec as P

MESH = pl.DeviceIdType.MESH
HIGHEST = lax.Precision.HIGHEST
F32 = jnp.float32
BF16 = jnp.bfloat16


def nn(a, b, precision=None):
    return lax.dot_general(a, b, (((1,), (0,)), ((), ())), precision=precision, preferred_element_type=F32)


def nt(a, b, precision=None):
    return lax.dot_general(a, b, (((1,), (1,)), ((), ())), precision=precision, preferred_element_type=F32)


def tn(a, b, precision=None):
    return lax.dot_general(a, b, (((0,), (0,)), ((), ())), precision=precision, preferred_element_type=F32)


def iota(shape, dim):
    return lax.broadcasted_iota(jnp.int32, shape, dim)


def exchange_in_kernel(n, heads, *refs):
    (u, w1, r1, w2, r2, g1, g2, o1, o2, ct) = refs[:10]
    (u_all, w1_all, r1_all, w2_all, r2_all, g1_all, g2_all, o1_all, o2_all, ct_all) = refs[10:20]
    ct_low, send, recv = refs[20:]
    me = lax.axis_index("seq")
    width = u.shape[1] // n
    barrier = pltpu.get_barrier_semaphore()
    for d in range(1, n):
        pl.semaphore_signal(barrier, inc=1, device_id={"seq": lax.rem(me + d, n)}, device_id_type=MESH)
    ct_low[...] = ct[...].astype(BF16)
    pl.semaphore_wait(barrier, n - 1)

    def cut(ref, at):
        return ref.at[:, pl.ds(pl.multiple_of(at * width, width), width)]

    copies = []
    for d in range(1, n):
        to = lax.rem(me + d, n)
        pairs = [
            (g1.at[to], g1_all.at[me]),
            (g2.at[to], g2_all.at[me]),
            (w1, w1_all.at[me]),
            (r1, r1_all.at[me]),
            (w2, w2_all.at[me]),
            (r2, r2_all.at[me]),
            (o1, o1_all.at[me]),
            (o2, o2_all.at[me]),
            (cut(u, to), u_all.at[me]),
            (cut(ct_low, to), ct_all.at[me]),
        ]
        for k, (src, dst) in enumerate(pairs):
            copy = pltpu.make_async_remote_copy(
                src_ref=src,
                dst_ref=dst,
                send_sem=send.at[d - 1, k],
                recv_sem=recv.at[d - 1, k],
                device_id={"seq": to},
                device_id_type=MESH,
            )
            copy.start()
            copies.append(copy)
    g1_all[me] = g1[me]
    g2_all[me] = g2[me]
    w1_all[me] = w1[...]
    r1_all[me] = r1[...]
    w2_all[me] = w2[...]
    r2_all[me] = r2[...]
    o1_all[me] = o1[...]
    o2_all[me] = o2[...]
    here = pl.ds(pl.multiple_of(me * width, width), width)
    u_all[me] = u[:, here]
    ct_all[me] = ct_low[:, here]
    for copy in copies:
        copy.wait()


def exchange_in(n, u, w1, r1, w2, r2, g1, g2, o1, o2, ct):
    length, features = u.shape
    heads = g1.shape[1]

    def out(*shape, dtype):
        return jax.ShapeDtypeStruct((n,) + shape, dtype)

    states = w1.shape[1]
    vmem = pl.BlockSpec(memory_space=pltpu.VMEM)
    return pl.pallas_call(
        functools.partial(exchange_in_kernel, n, heads),
        out_shape=(
            out(length, features // n, dtype=BF16),
            out(length, states, dtype=BF16),
            out(length, states, dtype=BF16),
            out(length, states, dtype=BF16),
            out(length, states, dtype=BF16),
            out(heads, length, dtype=F32),
            out(heads, length, dtype=F32),
            out(1, length, dtype=jnp.int32),
            out(1, length, dtype=jnp.int32),
            out(length, features // n, dtype=BF16),
        ),
        in_specs=[vmem] * 10,
        out_specs=[vmem] * 10,
        scratch_shapes=[
            pltpu.VMEM((length, features), BF16),
            pltpu.SemaphoreType.DMA((n - 1, 10)),
            pltpu.SemaphoreType.DMA((n - 1, 10)),
        ],
        compiler_params=pltpu.CompilerParams(collective_id=0, has_side_effects=True),
        name="exchange_in",
    )(u, w1, r1, w2, r2, g1, g2, o1, o2, ct)


def spread(x, size):
    per = 128 // size
    rows, heads = x.shape
    lane = iota((rows, 128), 1) // size
    parts = []
    for j in range(heads // per):
        part = jnp.broadcast_to(x[:, per * j : per * j + 1], (rows, 128))
        for k in range(1, per):
            part = jnp.where(lane == k, x[:, per * j + k : per * j + k + 1], part)
        parts.append(part)
    return jnp.concatenate(parts, axis=1)


def split_heads(x, size):
    lane = iota(x.shape, 1) // size
    return jnp.concatenate([jnp.where(lane == k, x, jnp.zeros_like(x)) for k in range(128 // size)], axis=0)


def scale_rows(state, factor, size):
    heads = factor.shape[0]
    return jnp.concatenate(
        [state[h * size : (h + 1) * size] * factor[h : h + 1] for h in range(heads)], axis=0
    )


class Chunk:
    def __init__(self, log_decay, size):
        heads, length = log_decay.shape
        self.size, self.heads, self.length = size, heads, length
        before = (iota((length, length), 0) <= iota((length, length), 1)).astype(F32)
        after = (iota((length, length), 1) <= iota((length, length), 0)).astype(F32)
        self.row = nn(log_decay, before, HIGHEST)
        self.col = nt(after, log_decay, HIGHEST)
        total = self.col[length - 1 : length, :]
        self.grown = jnp.exp(self.col)
        self.left = jnp.exp(total - self.col)
        self.total = jnp.exp(self.row[:, length - 1 : length])

    def gaps(self, h):
        gap = self.col[:, h : h + 1] - self.row[h : h + 1, :]
        causal = iota(gap.shape, 0) >= iota(gap.shape, 1)
        return jnp.where(causal, jnp.exp(jnp.minimum(gap, 0.0)), 0.0)

    def gaps_turned(self, h):
        gap = self.row[h : h + 1, :] - self.col[:, h : h + 1]
        causal = iota(gap.shape, 0) <= iota(gap.shape, 1)
        return jnp.where(causal, jnp.exp(jnp.minimum(gap, 0.0)), 0.0)


def layer_forward(u, w, r, chunk, skip, state):
    size = chunk.size
    per = 128 // size
    scores = nt(r, w)
    outputs = []
    for j in range(chunk.heads // per):
        weights = jnp.concatenate(
            [(chunk.gaps(per * j + k) * scores).astype(BF16) for k in range(per)], axis=1
        )
        outputs.append(nn(weights, split_heads(u[:, 128 * j : 128 * (j + 1)], size)))
    wide = u.astype(F32)
    y = jnp.concatenate(outputs, axis=1) + spread(chunk.grown, size) * nt(r, state.astype(BF16)) + skip * wide
    scaled = (wide * spread(chunk.left, size)).astype(BF16)
    return y, scale_rows(state, chunk.total, size) + tn(scaled, w)


def layer_back(dy, w, r, chunk, skip, adjoint):
    size = chunk.size
    per = 128 // size
    scores = nt(w, r)
    outputs = []
    for j in range(chunk.heads // per):
        weights = jnp.concatenate(
            [(chunk.gaps_turned(per * j + k) * scores).astype(BF16) for k in range(per)], axis=1
        )
        outputs.append(nn(weights, split_heads(dy[:, 128 * j : 128 * (j + 1)], size)))
    wide = dy.astype(F32)
    du = jnp.concatenate(outputs, axis=1) + spread(chunk.left, size) * nt(w, adjoint.astype(BF16)) + skip * wide
    scaled = (wide * spread(chunk.grown, size)).astype(BF16)
    return du, scale_rows(adjoint, chunk.total, size) + tn(scaled, r)


def layer_grads(u, dy, w, r, chunk, skip, state, adjoint, want_input):
    size, heads, length = chunk.size, chunk.heads, chunk.length
    per = 128 // size
    features = heads * size
    scores = nt(w, r)
    since = (iota((length, length), 0) >= iota((length, length), 1)).astype(BF16)
    earlier = iota((length, length), 0) < iota((length, length), 1)
    picks = (iota((heads, features), 1) // size == iota((heads, features), 0)).astype(BF16)
    dscores = jnp.zeros((length, length), F32)
    rows, outputs = [], []
    for j in range(heads // per):
        lanes = slice(128 * j, 128 * (j + 1))
        crossed = nt(split_heads(u[:, lanes], size), dy[:, lanes])
        moved, weights = [], []
        for k in range(per):
            gap = chunk.gaps_turned(per * j + k)
            part = gap * crossed[k * length : (k + 1) * length]
            dscores = dscores + part
            moved.append((part * scores).astype(BF16))
            if want_input:
                weights.append((gap * scores).astype(BF16))
        sums = nn(jnp.concatenate(moved, axis=0), since)
        for k in range(per):
            rows.append(
                jnp.sum(
                    jnp.where(earlier, sums[k * length : (k + 1) * length], 0.0), axis=0, keepdims=True
                )
            )
        if want_input:
            outputs.append(nn(jnp.concatenate(weights, axis=1), split_heads(dy[:, lanes], size)))
    wide_u, wide_dy = u.astype(F32), dy.astype(F32)
    left = spread(chunk.left, size)
    dy_scaled = wide_dy * spread(chunk.grown, size)
    u_scaled = wide_u * left
    dy_low, u_low = dy_scaled.astype(BF16), u_scaled.astype(BF16)
    state_low, adjoint_low = state.astype(BF16), adjoint.astype(BF16)
    dscores = dscores.astype(BF16)
    dreads = tn(dscores, w) + nn(dy_low, state_low)
    dwrites = nn(dscores, r) + nn(u_low, adjoint_low)
    read = nt(r, state_low)
    back = nt(w, adjoint_low)
    come = nt(picks, (dy_scaled * read).astype(BF16))
    gone = nt(picks, (u_scaled * back).astype(BF16))
    through = jnp.sum(nn(picks, (state * adjoint).astype(BF16)), axis=1, keepdims=True) * chunk.total
    ddecay = (
        jnp.concatenate(rows, axis=0)
        + nn(come.astype(BF16), since)
        + nn(gone.astype(BF16), earlier.astype(BF16))
        + through
    )
    dskip = jnp.sum(wide_u * wide_dy, axis=0, keepdims=True)
    if want_input:
        du = jnp.concatenate(outputs, axis=1) + left * back + skip * wide_dy
        return dwrites, dreads, ddecay, dskip, du, scale_rows(adjoint, chunk.total, size) + tn(dy_low, r)
    return dwrites, dreads, ddecay, dskip, None, scale_rows(state, chunk.total, size) + tn(u_low, w)


def compute_kernel(n, size, *refs):
    (u1, w1, r1, w2, r2, g1, g2, o1, o2, ct, k1, k2) = refs[:12]
    (du1, params, decays, skips) = refs[12:16]
    (y1, du2, u2, dy1, states, adjoints, state, adjoint) = refs[16:]
    heads, length = g1.shape[1:]
    features = u1.shape[2]
    first = lax.axis_index("seq") * heads

    def gains(ref):
        channel = iota((1, features), 1) // size
        row = jnp.zeros((1, features), F32)
        for h in range(heads):
            row = jnp.where(channel == h, ref[first + h], row)
        return row

    skip1, skip2 = gains(k1), gains(k2)
    state[...] = jnp.zeros_like(state)
    adjoint[...] = jnp.zeros_like(adjoint)

    def outer(i, carry):
        b = n - 1 - i
        states[i] = state[...]
        y, new = layer_forward(u1[i], w1[i], r1[i], Chunk(g1[i], size), skip1, state[...])
        y1[i] = y.astype(BF16)
        state[...] = new
        adjoints[b] = adjoint[...]
        du, new = layer_back(ct[b], w2[b], r2[b], Chunk(g2[b], size), skip2, adjoint[...])
        du2[b] = du.astype(BF16)
        adjoint[...] = new
        return carry

    lax.fori_loop(0, n, outer, 0)

    def regrid(i, carry):
        second = jnp.transpose(jnp.broadcast_to(o2[i].astype(F32), (length, length)))
        first_cells = jnp.transpose(jnp.broadcast_to(o1[i].astype(F32), (length, length)))
        forward = jnp.zeros((length, features), F32)
        back = jnp.zeros((length, features), F32)
        for j in range(n):
            take = (second == o1[j].astype(F32)).astype(BF16)
            forward = forward + nn(take, y1[j])
            take = (first_cells == o2[j].astype(F32)).astype(BF16)
            back = back + nn(take, du2[j])
        u2[i] = forward.astype(BF16)
        dy1[i] = back.astype(BF16)
        return carry

    lax.fori_loop(0, n, regrid, 0)
    state[...] = jnp.zeros_like(state)
    adjoint[...] = jnp.zeros_like(adjoint)
    skips[...] = jnp.zeros_like(skips)

    def inner(i, carry):
        b = n - 1 - i
        dw, dr, dg, dk, _, new = layer_grads(
            u2[i], ct[i], w2[i], r2[i], Chunk(g2[i], size), skip2, state[...], adjoints[i], False
        )
        state[...] = new
        params[i, 2] = dw.astype(params.dtype)
        params[i, 3] = dr.astype(params.dtype)
        decays[i, 1] = dg
        skips[1:2, :] += dk
        dw, dr, dg, dk, du, new = layer_grads(
            u1[b], dy1[b], w1[b], r1[b], Chunk(g1[b], size), skip1, states[b], adjoint[...], True
        )
        adjoint[...] = new
        du1[b] = du.astype(BF16)
        params[b, 0] = dw.astype(params.dtype)
        params[b, 1] = dr.astype(params.dtype)
        decays[b, 0] = dg
        skips[0:1, :] += dk
        return carry

    lax.fori_loop(0, n, inner, 0)


def compute(n, size, u, w1, r1, w2, r2, g1, g2, o1, o2, ct, k1, k2):
    _, length, features = u.shape
    heads = g1.shape[1]
    states = w1.shape[2]
    vmem = pl.BlockSpec(memory_space=pltpu.VMEM)
    smem = pl.BlockSpec(memory_space=pltpu.SMEM)
    return pl.pallas_call(
        functools.partial(compute_kernel, n, size),
        out_shape=(
            jax.ShapeDtypeStruct((n, length, features), BF16),
            jax.ShapeDtypeStruct((n, 4, length, states), BF16),
            jax.ShapeDtypeStruct((n, 2, heads, length), F32),
            jax.ShapeDtypeStruct((2, features), F32),
        ),
        in_specs=[vmem] * 10 + [smem] * 2,
        out_specs=[vmem] * 4,
        scratch_shapes=[pltpu.VMEM((n, length, features), BF16)] * 4
        + [pltpu.VMEM((n, features, states), F32)] * 2
        + [pltpu.VMEM((features, states), F32)] * 2,
        name="compute",
    )(u, w1, r1, w2, r2, g1, g2, o1, o2, ct, k1, k2)


def exchange_out_kernel(n, clips, factor, *refs):
    (du, params, decays, skips) = refs[:4]
    (dinput, dw1, dr1, dw2, dr2, dg1, dg2, dk1, dk2) = refs[4:13]
    (params_in, decays_in, clips_in, summed, parts_in, send, recv, clip_send, clip_recv) = refs[13:]
    me, clip = lax.axis_index("seq"), lax.axis_index("dp")
    width = du.shape[2]
    heads = decays.shape[2]
    size = width // heads
    barrier = pltpu.get_barrier_semaphore()
    for d in range(1, n):
        pl.semaphore_signal(barrier, inc=1, device_id={"seq": lax.rem(me + d, n)}, device_id_type=MESH)
    for d in range(1, clips):
        pl.semaphore_signal(barrier, inc=1, device_id={"dp": lax.rem(clip + d, clips)}, device_id_type=MESH)
    pl.semaphore_wait(barrier, n + clips - 2)

    def send_to(axis, to, src, dst, one, two):
        copy = pltpu.make_async_remote_copy(
            src_ref=src, dst_ref=dst, send_sem=one, recv_sem=two, device_id={axis: to}, device_id_type=MESH
        )
        copy.start()
        return copy

    clip_copies = []
    for d in range(1, clips):
        to = lax.rem(clip + d, clips)
        clip_copies.append(send_to("dp", to, skips, clips_in.at[clip], clip_send.at[d - 1], clip_recv.at[d - 1]))
    here = pl.ds(pl.multiple_of(me * width, width), width)
    copies = []
    for d in range(1, n):
        to = lax.rem(me + d, n)
        for k, (src, dst) in enumerate(
            [(params.at[to], params_in.at[me]), (decays.at[to], decays_in.at[me]), (du.at[to], dinput.at[:, here])]
        ):
            copies.append(send_to("seq", to, src, dst, send.at[d - 1, k], recv.at[d - 1, k]))
    clips_in[clip] = skips[...]
    params_in[me] = params[me]
    decays_in[me] = decays[me]
    dinput[:, here] = du[me]
    for copy in clip_copies:
        copy.wait()
    summed[...] = jnp.sum(clips_in[...], axis=0)
    parts_in[me] = summed[...]
    for d in range(1, n):
        to = lax.rem(me + d, n)
        copies.append(send_to("seq", to, summed, parts_in.at[me], send.at[d - 1, 3], recv.at[d - 1, 3]))
    for copy in copies:
        copy.wait()
    for k, out in enumerate((dw1, dr1, dw2, dr2)):
        total = params_in[0, k].astype(F32)
        for s in range(1, n):
            total = total + params_in[s, k].astype(F32)
        out[...] = total.astype(BF16)
    picks = (iota((width, heads), 0) // size == iota((width, heads), 1)).astype(F32)
    for s in range(n):
        dg1[s] = decays_in[s, 0]
        dg2[s] = decays_in[s, 1]
        by_head = nn(parts_in[s], picks, HIGHEST) * factor
        dk1[:, s * heads : (s + 1) * heads] = by_head[0:1]
        dk2[:, s * heads : (s + 1) * heads] = by_head[1:2]


def exchange_out(n, clips, factor, du, params, decays, skips):
    _, length, features = du.shape
    states = params.shape[3]
    heads = decays.shape[2]
    vmem = pl.BlockSpec(memory_space=pltpu.VMEM)
    param = jax.ShapeDtypeStruct((length, states), BF16)
    decay = jax.ShapeDtypeStruct((n, heads, length), F32)
    skip = jax.ShapeDtypeStruct((1, n * heads), F32)
    return pl.pallas_call(
        functools.partial(exchange_out_kernel, n, clips, factor),
        out_shape=(jax.ShapeDtypeStruct((length, n * features), BF16),) + (param,) * 4 + (decay,) * 2 + (skip,) * 2,
        in_specs=[vmem] * 4,
        out_specs=[vmem] * 9,
        scratch_shapes=[
            pltpu.VMEM(params.shape, params.dtype),
            pltpu.VMEM(decays.shape, F32),
            pltpu.VMEM((clips, 2, features), F32),
            pltpu.VMEM((2, features), F32),
            pltpu.VMEM((n, 2, features), F32),
            pltpu.SemaphoreType.DMA((n - 1, 4)),
            pltpu.SemaphoreType.DMA((n - 1, 4)),
            pltpu.SemaphoreType.DMA((clips - 1,)),
            pltpu.SemaphoreType.DMA((clips - 1,)),
        ],
        compiler_params=pltpu.CompilerParams(collective_id=1, has_side_effects=True),
        name="exchange_out",
    )(du, params, decays, skips)


def on_device(n, clips, u, w1, r1, g1, k1, w2, r2, g2, k2, o1, o2, ct):
    length, features = u.shape[1:]
    head_count = k1.shape[0]
    size = features // head_count
    heads = head_count // n

    def by_device(g):
        return g.reshape(n, heads, length)

    arrived = exchange_in(
        n, u[0], w1[0], r1[0], w2[0], r2[0], by_device(g1), by_device(g2), o1[None], o2[None], ct[0]
    )
    results = compute(n, size, *arrived, k1, k2)
    factor = 1.0 / math.sqrt(clips * n * length * size)
    du, dw1, dr1, dw2, dr2, dg1, dg2, dk1, dk2 = exchange_out(n, clips, factor, *results)
    return (
        du[None],
        dw1[None],
        dr1[None],
        dg1.reshape(1, head_count, length),
        dk1[0],
        dw2[None],
        dr2[None],
        dg2.reshape(1, head_count, length),
        dk2[0],
    )


def solution(mesh):
    tokens, decay = P("dp", "seq", None), P("dp", None, "seq")
    return jax.shard_map(
        functools.partial(on_device, mesh.shape["seq"], mesh.shape["dp"]),
        mesh=mesh,
        in_specs=(tokens, tokens, tokens, decay, P(), tokens, tokens, decay, P(), P("seq"), P("seq"), tokens),
        out_specs=(tokens, tokens, tokens, decay, P(), tokens, tokens, decay, P()),
        check_vma=False,
    )
```

```python
import functools
import math

import jax
import jax.numpy as jnp
from jax import lax
from jax.experimental import pallas as pl
from jax.experimental.pallas import tpu as pltpu
from jax.sharding import PartitionSpec as P

MESH = pl.DeviceIdType.MESH
HIGHEST = lax.Precision.HIGHEST
F32 = jnp.float32
BF16 = jnp.bfloat16


def nn(a, b, precision=None):
    return lax.dot_general(a, b, (((1,), (0,)), ((), ())), precision=precision, preferred_element_type=F32)


def nt(a, b, precision=None):
    return lax.dot_general(a, b, (((1,), (1,)), ((), ())), precision=precision, preferred_element_type=F32)


def tn(a, b, precision=None):
    return lax.dot_general(a, b, (((0,), (0,)), ((), ())), precision=precision, preferred_element_type=F32)


def iota(shape, dim):
    return lax.broadcasted_iota(jnp.int32, shape, dim)


def two(a):
    high = a.astype(BF16)
    return high, (a - high.astype(F32)).astype(BF16)


def nn2(a, b):
    high, low = two(a)
    return nn(high, b) + nn(low, b)


def nt2(a, b):
    high, low = two(b)
    return nt(a, high) + nt(a, low)


def tn2(a, b):
    high, low = two(a)
    return tn(high, b) + tn(low, b)


def spread(x, size):
    per = 128 // size
    rows, heads = x.shape
    lane = iota((rows, 128), 1) // size
    parts = []
    for j in range(heads // per):
        part = jnp.broadcast_to(x[:, per * j : per * j + 1], (rows, 128))
        for k in range(1, per):
            part = jnp.where(lane == k, x[:, per * j + k : per * j + k + 1], part)
        parts.append(part)
    return jnp.concatenate(parts, axis=1)


def split_heads(x, size):
    lane = iota(x.shape, 1) // size
    return jnp.concatenate([jnp.where(lane == k, x, jnp.zeros_like(x)) for k in range(128 // size)], axis=0)


def scale_rows(state, factor, size):
    heads = factor.shape[0]
    return jnp.concatenate(
        [state[h * size : (h + 1) * size] * factor[h : h + 1] for h in range(heads)], axis=0
    )


class Chunk:
    def __init__(self, log_decay, size):
        heads, length = log_decay.shape
        self.size, self.heads, self.length = size, heads, length
        before = (iota((length, length), 0) <= iota((length, length), 1)).astype(F32)
        after = (iota((length, length), 1) <= iota((length, length), 0)).astype(F32)
        self.row = nn(log_decay, before, HIGHEST)
        self.col = nt(after, log_decay, HIGHEST)
        total = self.col[length - 1 : length, :]
        self.grown = jnp.exp(self.col)
        self.left = jnp.exp(total - self.col)
        self.total = jnp.exp(self.row[:, length - 1 : length])

    def gaps(self, h):
        gap = self.col[:, h : h + 1] - self.row[h : h + 1, :]
        causal = iota(gap.shape, 0) >= iota(gap.shape, 1)
        return jnp.where(causal, jnp.exp(jnp.minimum(gap, 0.0)), 0.0)

    def gaps_turned(self, h):
        gap = self.row[h : h + 1, :] - self.col[:, h : h + 1]
        causal = iota(gap.shape, 0) <= iota(gap.shape, 1)
        return jnp.where(causal, jnp.exp(jnp.minimum(gap, 0.0)), 0.0)


def layer_forward(u, w, r, chunk, skip, state):
    size = chunk.size
    per = 128 // size
    scores = nt(r, w)
    outputs = []
    for j in range(chunk.heads // per):
        weights = jnp.concatenate(
            [chunk.gaps(per * j + k) * scores for k in range(per)], axis=1
        )
        outputs.append(nn2(weights, split_heads(u[:, 128 * j : 128 * (j + 1)], size)))
    wide = u.astype(F32)
    y = jnp.concatenate(outputs, axis=1) + spread(chunk.grown, size) * nt2(r, state) + skip * wide
    scaled = wide * spread(chunk.left, size)
    return y, scale_rows(state, chunk.total, size) + tn2(scaled, w)


def layer_back(dy, w, r, chunk, skip, adjoint):
    size = chunk.size
    per = 128 // size
    scores = nt(w, r)
    outputs = []
    for j in range(chunk.heads // per):
        weights = jnp.concatenate(
            [chunk.gaps_turned(per * j + k) * scores for k in range(per)], axis=1
        )
        outputs.append(nn2(weights, split_heads(dy[:, 128 * j : 128 * (j + 1)], size)))
    wide = dy.astype(F32)
    du = jnp.concatenate(outputs, axis=1) + spread(chunk.left, size) * nt2(w, adjoint) + skip * wide
    scaled = wide * spread(chunk.grown, size)
    return du, scale_rows(adjoint, chunk.total, size) + tn2(scaled, r)


def layer_grads(u, dy, w, r, chunk, skip, state, adjoint, want_input):
    size, heads, length = chunk.size, chunk.heads, chunk.length
    per = 128 // size
    features = heads * size
    scores = nt(w, r)
    since = (iota((length, length), 0) >= iota((length, length), 1)).astype(BF16)
    earlier = iota((length, length), 0) < iota((length, length), 1)
    picks = (iota((heads, features), 1) // size == iota((heads, features), 0)).astype(BF16)
    dscores = jnp.zeros((length, length), F32)
    rows, outputs = [], []
    for j in range(heads // per):
        lanes = slice(128 * j, 128 * (j + 1))
        crossed = nt(split_heads(u[:, lanes], size), dy[:, lanes])
        moved, weights = [], []
        for k in range(per):
            gap = chunk.gaps_turned(per * j + k)
            part = gap * crossed[k * length : (k + 1) * length]
            dscores = dscores + part
            moved.append((part * scores).astype(BF16))
            if want_input:
                weights.append((gap * scores).astype(BF16))
        sums = nn(jnp.concatenate(moved, axis=0), since)
        for k in range(per):
            rows.append(
                jnp.sum(
                    jnp.where(earlier, sums[k * length : (k + 1) * length], 0.0), axis=0, keepdims=True
                )
            )
        if want_input:
            outputs.append(nn(jnp.concatenate(weights, axis=1), split_heads(dy[:, lanes], size)))
    wide_u, wide_dy = u.astype(F32), dy.astype(F32)
    left = spread(chunk.left, size)
    dy_scaled = wide_dy * spread(chunk.grown, size)
    u_scaled = wide_u * left
    dy_low, u_low = dy_scaled.astype(BF16), u_scaled.astype(BF16)
    state_low, adjoint_low = state.astype(BF16), adjoint.astype(BF16)
    dscores = dscores.astype(BF16)
    dreads = tn(dscores, w) + nn(dy_low, state_low)
    dwrites = nn(dscores, r) + nn(u_low, adjoint_low)
    read = nt(r, state_low)
    back = nt(w, adjoint_low)
    come = nt(picks, (dy_scaled * read).astype(BF16))
    gone = nt(picks, (u_scaled * back).astype(BF16))
    through = jnp.sum(nn(picks, (state * adjoint).astype(BF16)), axis=1, keepdims=True) * chunk.total
    ddecay = (
        jnp.concatenate(rows, axis=0)
        + nn(come.astype(BF16), since)
        + nn(gone.astype(BF16), earlier.astype(BF16))
        + through
    )
    if want_input:
        du = jnp.concatenate(outputs, axis=1) + left * back + skip * wide_dy
        return dwrites, dreads, ddecay, du, scale_rows(adjoint, chunk.total, size) + tn(dy_low, r)
    return dwrites, dreads, ddecay, None, scale_rows(state, chunk.total, size) + tn(u_low, w)


def whole_kernel(n, clips, size, *refs):
    (u, w1, r1, g1, k1, w2, r2, g2, k2, o1, o2, ct) = refs[:12]
    (dinput, params1_in, params2_in, decays1_in, decays2_in, parts_in) = refs[12:18]
    (u1, w1_all, r1_all, g1_all, w2_all, r2_all, g2_all, o1_all, o2_all, ct_high, ct_low) = refs[18:29]
    (high_out, low_out, y1, du2_high, du2, u2, dy1, states, adjoints, state, adjoint) = refs[29:40]
    (du1, params1, params2, decays1, decays2, skips, clips_in, summed) = refs[40:48]
    (send, recv, out_send, out_recv, clip_send, clip_recv) = refs[48:]
    me, clip = lax.axis_index("seq"), lax.axis_index("dp")
    heads, length = g1.shape[1:]
    features = heads * size
    here = pl.ds(pl.multiple_of(me * features, features), features)

    barrier = pltpu.get_barrier_semaphore()
    for d in range(1, n):
        pl.semaphore_signal(barrier, inc=1, device_id={"seq": lax.rem(me + d, n)}, device_id_type=MESH)
    for d in range(1, clips):
        pl.semaphore_signal(barrier, inc=1, device_id={"dp": lax.rem(clip + d, clips)}, device_id_type=MESH)
    high, low = two(ct[...])
    high_out[...] = high
    low_out[...] = low
    pl.semaphore_wait(barrier, n + clips - 2)

    def copy_to(axis, to, src, dst, one, other):
        return pltpu.make_async_remote_copy(
            src_ref=src, dst_ref=dst, send_sem=one, recv_sem=other, device_id={axis: to}, device_id_type=MESH
        )

    def cut(ref, at):
        return ref.at[:, pl.ds(pl.multiple_of(at * features, features), features)]

    moves = [
        lambda to: (g2.at[to], g2_all.at[me]),
        lambda to: (w2, w2_all.at[me]),
        lambda to: (r2, r2_all.at[me]),
        lambda to: (cut(high_out, to), ct_high.at[me]),
        lambda to: (g1.at[to], g1_all.at[me]),
        lambda to: (w1, w1_all.at[me]),
        lambda to: (r1, r1_all.at[me]),
        lambda to: (cut(u, to), u1.at[me]),
        lambda to: (o1, o1_all.at[me]),
        lambda to: (o2, o2_all.at[me]),
        lambda to: (cut(low_out, to), ct_low.at[me]),
    ]
    arriving = []
    for k, move in enumerate(moves):
        arriving.append([])
        for d in range(1, n):
            to = lax.rem(me + d, n)
            src, dst = move(to)
            copy = copy_to("seq", to, src, dst, send.at[d - 1, k], recv.at[d - 1, k])
            copy.start()
            arriving[k].append(copy)
    for src, dst in ((g1, g1_all), (g2, g2_all)):
        dst[me] = src[me]
    for src, dst in ((w1, w1_all), (r1, r1_all), (w2, w2_all), (r2, r2_all), (o1, o1_all), (o2, o2_all)):
        dst[me] = src[...]
    u1[me] = u[:, here]
    ct_high[me] = high_out[:, here]
    ct_low[me] = low_out[:, here]

    first = me * heads

    def gains(ref):
        channel = iota((1, features), 1) // size
        row = jnp.zeros((1, features), F32)
        for h in range(heads):
            row = jnp.where(channel == h, ref[first + h], row)
        return row

    skip1, skip2 = gains(k1), gains(k2)
    state[...] = jnp.zeros_like(state)
    adjoint[...] = jnp.zeros_like(adjoint)

    for k in range(0, 4):
        for copy in arriving[k]:
            copy.wait_recv()

    def back_second(i, carry):
        b = n - 1 - i
        adjoints[b] = adjoint[...]
        du, new = layer_back(ct_high[b], w2_all[b], r2_all[b], Chunk(g2_all[b], size), skip2, adjoint[...])
        du2_high[b] = du
        adjoint[...] = new
        return carry

    lax.fori_loop(0, n, back_second, 0)
    for k in range(4, 8):
        for copy in arriving[k]:
            copy.wait_recv()

    def forward_first(i, carry):
        states[i] = state[...]
        y, new = layer_forward(u1[i], w1_all[i], r1_all[i], Chunk(g1_all[i], size), skip1, state[...])
        y1[i] = y.astype(BF16)
        state[...] = new
        return carry

    lax.fori_loop(0, n, forward_first, 0)
    for k in range(8, 11):
        for copy in arriving[k]:
            copy.wait_recv()

    def finish_back(i, carry):
        du2[i] = (du2_high[i] + skip2 * ct_low[i].astype(F32)).astype(BF16)
        return carry

    lax.fori_loop(0, n, finish_back, 0)
    skips[...] = jnp.zeros_like(skips)

    def regrid(i, carry):
        second = jnp.transpose(jnp.broadcast_to(o2_all[i].astype(F32), (length, length)))
        first_cells = jnp.transpose(jnp.broadcast_to(o1_all[i].astype(F32), (length, length)))
        forward = jnp.zeros((length, features), F32)
        back = jnp.zeros((length, features), F32)
        for j in range(n):
            take = (second == o1_all[j].astype(F32)).astype(BF16)
            forward = forward + nn(take, y1[j])
            take = (first_cells == o2_all[j].astype(F32)).astype(BF16)
            back = back + nn(take, du2[j])
        u2[i] = forward.astype(BF16)
        dy1[i] = back.astype(BF16)
        upstream = ct_high[i].astype(F32) + ct_low[i].astype(F32)
        skips[0:1, :] += jnp.sum(u1[i].astype(F32) * back, axis=0, keepdims=True)
        skips[1:2, :] += jnp.sum(upstream * forward, axis=0, keepdims=True)
        return carry

    lax.fori_loop(0, n, regrid, 0)
    clip_copies = []
    for d in range(1, clips):
        to = lax.rem(clip + d, clips)
        copy = copy_to("dp", to, skips, clips_in.at[clip], clip_send.at[d - 1], clip_recv.at[d - 1])
        copy.start()
        clip_copies.append(copy)
    clips_in[clip] = skips[...]
    state[...] = jnp.zeros_like(state)
    adjoint[...] = jnp.zeros_like(adjoint)

    def leave_second(to, slot):
        return [
            copy_to("seq", to, params2.at[to], params2_in.at[me], out_send.at[slot, 0], out_recv.at[slot, 0]),
            copy_to("seq", to, decays2.at[to], decays2_in.at[me], out_send.at[slot, 1], out_recv.at[slot, 1]),
        ]

    def leave_first(to, slot):
        return [
            copy_to("seq", to, du1.at[to], dinput.at[:, here], out_send.at[slot, 2], out_recv.at[slot, 2]),
            copy_to("seq", to, params1.at[to], params1_in.at[me], out_send.at[slot, 3], out_recv.at[slot, 3]),
            copy_to("seq", to, decays1.at[to], decays1_in.at[me], out_send.at[slot, 4], out_recv.at[slot, 4]),
        ]

    def grads(i, carry):
        b = n - 1 - i
        dw, dr, dg, _, new = layer_grads(
            u2[i], ct_high[i], w2_all[i], r2_all[i], Chunk(g2_all[i], size), skip2, state[...], adjoints[i], False
        )
        state[...] = new
        params2[i, 0] = dw.astype(BF16)
        params2[i, 1] = dr.astype(BF16)
        decays2[i] = dg

        @pl.when(i != me)
        def _():
            for copy in leave_second(i, lax.rem(i - me + n, n) - 1):
                copy.start()

        dw, dr, dg, du, new = layer_grads(
            u1[b], dy1[b], w1_all[b], r1_all[b], Chunk(g1_all[b], size), skip1, states[b], adjoint[...], True
        )
        adjoint[...] = new
        du1[b] = du.astype(BF16)
        params1[b, 0] = dw.astype(BF16)
        params1[b, 1] = dr.astype(BF16)
        decays1[b] = dg

        @pl.when(b != me)
        def _():
            for copy in leave_first(b, lax.rem(b - me + n, n) - 1):
                copy.start()

        return carry

    lax.fori_loop(0, n, grads, 0)
    for copy in clip_copies:
        copy.wait()
    summed[...] = jnp.sum(clips_in[...], axis=0)
    last = []
    for d in range(1, n):
        to = lax.rem(me + d, n)
        copy = copy_to("seq", to, summed, parts_in.at[me], out_send.at[d - 1, 5], out_recv.at[d - 1, 5])
        copy.start()
        last.append(copy)
    parts_in[me] = summed[...]
    params1_in[me] = params1[me]
    params2_in[me] = params2[me]
    decays1_in[me] = decays1[me]
    decays2_in[me] = decays2[me]
    dinput[:, here] = du1[me]
    for group in arriving:
        for copy in group:
            copy.wait_send()
    for d in range(1, n):
        to = lax.rem(me + d, n)
        last += leave_second(to, d - 1) + leave_first(to, d - 1)
    for copy in last:
        copy.wait()


def whole(n, clips, size, u, w1, r1, g1, k1, w2, r2, g2, k2, o1, o2, ct):
    length, width = u.shape
    heads = g1.shape[1]
    count = w1.shape[1]
    features = heads * size
    vmem = pl.BlockSpec(memory_space=pltpu.VMEM)
    smem = pl.BlockSpec(memory_space=pltpu.SMEM)
    wide, param, params = (n, length, features), (n, length, count), (n, 2, length, count)
    decay, order, gain = (n, heads, length), (n, 1, length), (2, features)
    outs = (((length, width), BF16), (params, BF16), (params, BF16), (decay, F32), (decay, F32), ((n,) + gain, F32))
    held = [
        (wide, BF16),
        (param, BF16),
        (param, BF16),
        (decay, F32),
        (param, BF16),
        (param, BF16),
        (decay, F32),
        (order, jnp.int32),
        (order, jnp.int32),
        (wide, BF16),
        (wide, BF16),
        ((length, width), BF16),
        ((length, width), BF16),
        (wide, BF16),
        (wide, F32),
        (wide, BF16),
        (wide, BF16),
        (wide, BF16),
        ((n, features, count), F32),
        ((n, features, count), F32),
        ((features, count), F32),
        ((features, count), F32),
        (wide, BF16),
        (params, BF16),
        (params, BF16),
        (decay, F32),
        (decay, F32),
        (gain, F32),
        ((clips,) + gain, F32),
        (gain, F32),
    ]
    return pl.pallas_call(
        functools.partial(whole_kernel, n, clips, size),
        out_shape=tuple(jax.ShapeDtypeStruct(*out) for out in outs),
        in_specs=[vmem] * 4 + [smem] + [vmem] * 3 + [smem] + [vmem] * 3,
        out_specs=[vmem] * 6,
        scratch_shapes=[pltpu.VMEM(*one) for one in held]
        + [pltpu.SemaphoreType.DMA((n - 1, 11))] * 2
        + [pltpu.SemaphoreType.DMA((n - 1, 6))] * 2
        + [pltpu.SemaphoreType.DMA((clips - 1,))] * 2,
        compiler_params=pltpu.CompilerParams(collective_id=0, has_side_effects=True),
        name="whole",
    )(u, w1, r1, g1, k1, w2, r2, g2, k2, o1, o2, ct)


def gather_kernel(n, factor, *refs):
    (du, params1, params2, decays1, decays2, parts) = refs[:6]
    (dinput, dw1, dr1, dg1, dk1, dw2, dr2, dg2, dk2) = refs[6:]
    heads = decays1.shape[1]
    width = parts.shape[2]
    size = width // heads
    dinput[...] = du[...]
    dg1[...] = decays1[...]
    dg2[...] = decays2[...]
    for params, outs in ((params1, (dw1, dr1)), (params2, (dw2, dr2))):
        for k, out in enumerate(outs):
            total = params[0, k].astype(F32)
            for s in range(1, n):
                total = total + params[s, k].astype(F32)
            out[...] = total.astype(BF16)
    picks = (iota((width, heads), 0) // size == iota((width, heads), 1)).astype(F32)
    for s in range(n):
        by_head = nn(parts[s], picks, HIGHEST) * factor
        dk1[:, s * heads : (s + 1) * heads] = by_head[0:1]
        dk2[:, s * heads : (s + 1) * heads] = by_head[1:2]


def gather(n, factor, du, params1, params2, decays1, decays2, parts):
    length, count = params1.shape[2:]
    heads = decays1.shape[1]
    vmem = pl.BlockSpec(memory_space=pltpu.VMEM)
    param = jax.ShapeDtypeStruct((length, count), BF16)
    decay = jax.ShapeDtypeStruct(decays1.shape, F32)
    skip = jax.ShapeDtypeStruct((1, n * heads), F32)
    layer = (param, param, decay, skip)
    return pl.pallas_call(
        functools.partial(gather_kernel, n, factor),
        out_shape=(jax.ShapeDtypeStruct(du.shape, BF16),) + layer + layer,
        in_specs=[vmem] * 6,
        out_specs=[vmem] * 9,
        name="gather",
    )(du, params1, params2, decays1, decays2, parts)


def on_device(n, clips, u, w1, r1, g1, k1, w2, r2, g2, k2, o1, o2, ct):
    length, features = u.shape[1:]
    head_count = k1.shape[0]
    size = features // head_count
    heads = head_count // n

    def by_device(g):
        return g.reshape(n, heads, length)

    results = whole(
        n,
        clips,
        size,
        u[0],
        w1[0],
        r1[0],
        by_device(g1),
        k1,
        w2[0],
        r2[0],
        by_device(g2),
        k2,
        o1[None],
        o2[None],
        ct[0],
    )
    factor = 1.0 / math.sqrt(clips * n * length * size)
    du, dw1, dr1, dg1, dk1, dw2, dr2, dg2, dk2 = gather(n, factor, *results)
    return (
        du[None],
        dw1[None],
        dr1[None],
        dg1.reshape(1, head_count, length),
        dk1[0],
        dw2[None],
        dr2[None],
        dg2.reshape(1, head_count, length),
        dk2[0],
    )


def solution(mesh):
    tokens, decay = P("dp", "seq", None), P("dp", None, "seq")
    return jax.shard_map(
        functools.partial(on_device, mesh.shape["seq"], mesh.shape["dp"]),
        mesh=mesh,
        in_specs=(tokens, tokens, tokens, decay, P(), tokens, tokens, decay, P(), P("seq"), P("seq"), tokens),
        out_specs=(tokens, tokens, tokens, decay, P(), tokens, tokens, decay, P()),
        check_vma=False,
    )
```

```python
import functools
import math

import jax
import jax.numpy as jnp
from jax import lax
from jax.experimental import pallas as pl
from jax.experimental.pallas import tpu as pltpu
from jax.sharding import PartitionSpec as P

MESH = pl.DeviceIdType.MESH
HIGHEST = lax.Precision.HIGHEST
F32 = jnp.float32
BF16 = jnp.bfloat16


def nn(a, b, precision=None):
    return lax.dot_general(a, b, (((1,), (0,)), ((), ())), precision=precision, preferred_element_type=F32)


def nt(a, b, precision=None):
    return lax.dot_general(a, b, (((1,), (1,)), ((), ())), precision=precision, preferred_element_type=F32)


def tn(a, b, precision=None):
    return lax.dot_general(a, b, (((0,), (0,)), ((), ())), precision=precision, preferred_element_type=F32)


def iota(shape, dim):
    return lax.broadcasted_iota(jnp.int32, shape, dim)


def two(a):
    high = a.astype(BF16)
    return high, (a - high.astype(F32)).astype(BF16)


def nn2(a, b):
    high, low = two(a)
    return nn(high, b) + nn(low, b)


def nt2(a, b):
    high, low = two(b)
    return nt(a, high) + nt(a, low)


def tn2(a, b):
    high, low = two(a)
    return tn(high, b) + tn(low, b)


def spread(x, size):
    per = 128 // size
    rows, heads = x.shape
    lane = iota((rows, 128), 1) // size
    parts = []
    for j in range(heads // per):
        part = jnp.broadcast_to(x[:, per * j : per * j + 1], (rows, 128))
        for k in range(1, per):
            part = jnp.where(lane == k, x[:, per * j + k : per * j + k + 1], part)
        parts.append(part)
    return jnp.concatenate(parts, axis=1)


def split_heads(x, size):
    lane = iota(x.shape, 1) // size
    return jnp.concatenate([jnp.where(lane == k, x, jnp.zeros_like(x)) for k in range(128 // size)], axis=0)


def scale_rows(state, factor, size):
    heads = factor.shape[0]
    return jnp.concatenate(
        [state[h * size : (h + 1) * size] * factor[h : h + 1] for h in range(heads)], axis=0
    )


class Chunk:
    def __init__(self, log_decay, size):
        heads, length = log_decay.shape
        self.size, self.heads, self.length = size, heads, length
        before = (iota((length, length), 0) <= iota((length, length), 1)).astype(F32)
        after = (iota((length, length), 1) <= iota((length, length), 0)).astype(F32)
        self.row = nn(log_decay, before, HIGHEST)
        self.col = nt(after, log_decay, HIGHEST)
        total = self.col[length - 1 : length, :]
        self.grown = jnp.exp(self.col)
        self.left = jnp.exp(total - self.col)
        self.total = jnp.exp(self.row[:, length - 1 : length])

    def gaps(self, h):
        gap = self.col[:, h : h + 1] - self.row[h : h + 1, :]
        causal = iota(gap.shape, 0) >= iota(gap.shape, 1)
        return jnp.where(causal, jnp.exp(jnp.minimum(gap, 0.0)), 0.0)

    def gaps_turned(self, h):
        gap = self.row[h : h + 1, :] - self.col[:, h : h + 1]
        causal = iota(gap.shape, 0) <= iota(gap.shape, 1)
        return jnp.where(causal, jnp.exp(jnp.minimum(gap, 0.0)), 0.0)


def layer_forward(u, w, r, chunk, skip, state):
    size = chunk.size
    per = 128 // size
    scores = nt(r, w)
    outputs = []
    for j in range(chunk.heads // per):
        weights = jnp.concatenate(
            [chunk.gaps(per * j + k) * scores for k in range(per)], axis=1
        )
        outputs.append(nn2(weights, split_heads(u[:, 128 * j : 128 * (j + 1)], size)))
    wide = u.astype(F32)
    y = jnp.concatenate(outputs, axis=1) + spread(chunk.grown, size) * nt2(r, state) + skip * wide
    scaled = wide * spread(chunk.left, size)
    return y, scale_rows(state, chunk.total, size) + tn2(scaled, w)


def layer_back(dy, w, r, chunk, skip, adjoint):
    size = chunk.size
    per = 128 // size
    scores = nt(w, r)
    outputs = []
    for j in range(chunk.heads // per):
        weights = jnp.concatenate(
            [chunk.gaps_turned(per * j + k) * scores for k in range(per)], axis=1
        )
        outputs.append(nn2(weights, split_heads(dy[:, 128 * j : 128 * (j + 1)], size)))
    wide = dy.astype(F32)
    du = jnp.concatenate(outputs, axis=1) + spread(chunk.left, size) * nt2(w, adjoint) + skip * wide
    scaled = wide * spread(chunk.grown, size)
    return du, scale_rows(adjoint, chunk.total, size) + tn2(scaled, r)


def layer_grads(u, dy, w, r, chunk, skip, state, adjoint, want_input):
    size, heads, length = chunk.size, chunk.heads, chunk.length
    per = 128 // size
    features = heads * size
    scores = nt(w, r)
    since = (iota((length, length), 0) >= iota((length, length), 1)).astype(BF16)
    earlier = iota((length, length), 0) < iota((length, length), 1)
    picks = (iota((heads, features), 1) // size == iota((heads, features), 0)).astype(BF16)
    dscores = jnp.zeros((length, length), F32)
    rows, outputs = [], []
    for j in range(heads // per):
        lanes = slice(128 * j, 128 * (j + 1))
        crossed = nt(split_heads(u[:, lanes], size), dy[:, lanes])
        moved, weights = [], []
        for k in range(per):
            gap = chunk.gaps_turned(per * j + k)
            part = gap * crossed[k * length : (k + 1) * length]
            dscores = dscores + part
            moved.append((part * scores).astype(BF16))
            if want_input:
                weights.append((gap * scores).astype(BF16))
        sums = nn(jnp.concatenate(moved, axis=0), since)
        for k in range(per):
            rows.append(
                jnp.sum(
                    jnp.where(earlier, sums[k * length : (k + 1) * length], 0.0), axis=0, keepdims=True
                )
            )
        if want_input:
            outputs.append(nn(jnp.concatenate(weights, axis=1), split_heads(dy[:, lanes], size)))
    wide_u, wide_dy = u.astype(F32), dy.astype(F32)
    left = spread(chunk.left, size)
    dy_scaled = wide_dy * spread(chunk.grown, size)
    u_scaled = wide_u * left
    dy_low, u_low = dy_scaled.astype(BF16), u_scaled.astype(BF16)
    state_low, adjoint_low = state.astype(BF16), adjoint.astype(BF16)
    dscores = dscores.astype(BF16)
    dreads = tn(dscores, w) + nn(dy_low, state_low)
    dwrites = nn(dscores, r) + nn(u_low, adjoint_low)
    read = nt(r, state_low)
    back = nt(w, adjoint_low)
    come = nt(picks, (dy_scaled * read).astype(BF16))
    gone = nt(picks, (u_scaled * back).astype(BF16))
    through = jnp.sum(nn(picks, (state * adjoint).astype(BF16)), axis=1, keepdims=True) * chunk.total
    ddecay = (
        jnp.concatenate(rows, axis=0)
        + nn(come.astype(BF16), since)
        + nn(gone.astype(BF16), earlier.astype(BF16))
        + through
    )
    if want_input:
        du = jnp.concatenate(outputs, axis=1) + left * back + skip * wide_dy
        return dwrites, dreads, ddecay, du, scale_rows(adjoint, chunk.total, size) + tn(dy_low, r)
    return dwrites, dreads, ddecay, None, scale_rows(state, chunk.total, size) + tn(u_low, w)


def whole_kernel(n, clips, size, *refs):
    (u, w1, r1, g1, k1, w2, r2, g2, k2, o1, o2, ct) = refs[:12]
    (dinput, params1_in, params2_in, decays1_in, decays2_in, parts_in) = refs[12:18]
    (u1, w1_all, r1_all, g1_all, w2_all, r2_all, g2_all, o1_all, o2_all, ct_high, ct_low) = refs[18:29]
    (high_out, low_out, y1, du2_high, du2, u2, dy1, states, adjoints, state, adjoint) = refs[29:40]
    (du1, params1, params2, decays1, decays2, skips, clips_in, summed) = refs[40:48]
    (send, recv, out_send, out_recv, clip_send, clip_recv, near_send, near_recv) = refs[48:]
    me, clip = lax.axis_index("seq"), lax.axis_index("dp")
    heads, length = g1.shape[1:]
    features = heads * size
    here = pl.ds(pl.multiple_of(me * features, features), features)

    barrier = pltpu.get_barrier_semaphore()
    for d in range(1, n):
        pl.semaphore_signal(barrier, inc=1, device_id={"seq": lax.rem(me + d, n)}, device_id_type=MESH)
    for d in range(1, clips):
        pl.semaphore_signal(barrier, inc=1, device_id={"dp": lax.rem(clip + d, clips)}, device_id_type=MESH)
    high, low = two(ct[...])
    high_out[...] = high
    low_out[...] = low
    pl.semaphore_wait(barrier, n + clips - 2)

    def copy_to(axis, to, src, dst, one, other):
        return pltpu.make_async_remote_copy(
            src_ref=src, dst_ref=dst, send_sem=one, recv_sem=other, device_id={axis: to}, device_id_type=MESH
        )

    def cut(ref, at):
        return ref.at[:, pl.ds(pl.multiple_of(at * features, features), features)]

    moves = [
        lambda to: (g2.at[to], g2_all.at[me]),
        lambda to: (cut(high_out, to), ct_high.at[me]),
        lambda to: (g1.at[to], g1_all.at[me]),
        lambda to: (cut(u, to), u1.at[me]),
        lambda to: (o1, o1_all.at[me]),
        lambda to: (o2, o2_all.at[me]),
        lambda to: (cut(low_out, to), ct_low.at[me]),
    ]
    twin = me + 1 - 2 * lax.rem(me, 2)
    pairs = ((w2, w2_all), (r2, r2_all), (w1, w1_all), (r1, r1_all))
    far, near = [], []
    for k, (src, dst) in enumerate(pairs):
        for d in range(2, n, 2):
            at = d // 2 - 1
            copy = copy_to("seq", lax.rem(me + d, n), src, dst.at[me], near_send.at[at, k], near_recv.at[at, k])
            copy.start()
            far.append(copy)
        at = n // 2 - 1
        copy = copy_to("seq", twin, src, dst.at[me], near_send.at[at, k], near_recv.at[at, k])
        copy.start()
        near.append(copy)
    arriving = []
    for k, move in enumerate(moves):
        arriving.append([])
        for d in range(1, n):
            to = lax.rem(me + d, n)
            src, dst = move(to)
            copy = copy_to("seq", to, src, dst, send.at[d - 1, k], recv.at[d - 1, k])
            copy.start()
            arriving[k].append(copy)
    for src, dst in ((g1, g1_all), (g2, g2_all)):
        dst[me] = src[me]
    for src, dst in pairs + ((o1, o1_all), (o2, o2_all)):
        dst[me] = src[...]
    u1[me] = u[:, here]
    ct_high[me] = high_out[:, here]
    ct_low[me] = low_out[:, here]

    first = me * heads

    def gains(ref):
        channel = iota((1, features), 1) // size
        row = jnp.zeros((1, features), F32)
        for h in range(heads):
            row = jnp.where(channel == h, ref[first + h], row)
        return row

    skip1, skip2 = gains(k1), gains(k2)
    state[...] = jnp.zeros_like(state)
    adjoint[...] = jnp.zeros_like(adjoint)

    for copy in far:
        copy.wait_recv()
    for k, (src, dst) in enumerate(pairs):
        for d in range(2, n, 2):
            at, block = n // 2 + d // 2 - 1, lax.rem(me - d + n, n)
            copy = copy_to("seq", twin, dst.at[block], dst.at[block], near_send.at[at, k], near_recv.at[at, k])
            copy.start()
            near.append(copy)
    for copy in near:
        copy.wait_recv()
    for k in range(0, 2):
        for copy in arriving[k]:
            copy.wait_recv()

    def back_second(i, carry):
        b = n - 1 - i
        adjoints[b] = adjoint[...]
        du, new = layer_back(ct_high[b], w2_all[b], r2_all[b], Chunk(g2_all[b], size), skip2, adjoint[...])
        du2_high[b] = du
        adjoint[...] = new
        return carry

    lax.fori_loop(0, n, back_second, 0, unroll=2)
    for k in range(2, 4):
        for copy in arriving[k]:
            copy.wait_recv()

    def forward_first(i, carry):
        states[i] = state[...]
        y, new = layer_forward(u1[i], w1_all[i], r1_all[i], Chunk(g1_all[i], size), skip1, state[...])
        y1[i] = y.astype(BF16)
        state[...] = new
        return carry

    lax.fori_loop(0, n, forward_first, 0, unroll=2)
    for k in range(4, 6):
        for copy in arriving[k]:
            copy.wait_recv()

    def cells(ref, i):
        return jnp.transpose(jnp.broadcast_to(ref[i].astype(F32), (length, length)))

    def regrid(i, carry):
        second = cells(o2_all, i)
        total = jnp.zeros((length, features), F32)
        for j in range(n):
            take = (second == o1_all[j].astype(F32)).astype(BF16)
            total = total + nn(take, y1[j])
        u2[i] = total.astype(BF16)
        return carry

    lax.fori_loop(0, n, regrid, 0)

    state[...] = jnp.zeros_like(state)
    adjoint[...] = jnp.zeros_like(adjoint)

    def leave_second(to, slot):
        return [
            copy_to("seq", to, params2.at[to], params2_in.at[me], out_send.at[slot, 0], out_recv.at[slot, 0]),
            copy_to("seq", to, decays2.at[to], decays2_in.at[me], out_send.at[slot, 1], out_recv.at[slot, 1]),
        ]

    def leave_first(to, slot):
        return [
            copy_to("seq", to, du1.at[to], dinput.at[:, here], out_send.at[slot, 2], out_recv.at[slot, 2]),
            copy_to("seq", to, params1.at[to], params1_in.at[me], out_send.at[slot, 3], out_recv.at[slot, 3]),
            copy_to("seq", to, decays1.at[to], decays1_in.at[me], out_send.at[slot, 4], out_recv.at[slot, 4]),
        ]

    def grads_second(i, carry):
        dw, dr, dg, _, new = layer_grads(
            u2[i], ct_high[i], w2_all[i], r2_all[i], Chunk(g2_all[i], size), skip2, state[...], adjoints[i], False
        )
        state[...] = new
        params2[i, 0] = dw.astype(BF16)
        params2[i, 1] = dr.astype(BF16)
        decays2[i] = dg

        @pl.when(i != me)
        def _():
            for copy in leave_second(i, lax.rem(i - me + n, n) - 1):
                copy.start()

        return carry

    lax.fori_loop(0, n, grads_second, 0)
    for copy in arriving[6]:
        copy.wait_recv()
    skips[...] = jnp.zeros_like(skips)

    def finish_back(i, carry):
        rest = ct_low[i].astype(F32)
        du2[i] = (du2_high[i] + skip2 * rest).astype(BF16)
        upstream = ct_high[i].astype(F32) + rest
        skips[1:2, :] += jnp.sum(upstream * u2[i].astype(F32), axis=0, keepdims=True)
        return carry

    lax.fori_loop(0, n, finish_back, 0)

    def regrid_back(i, carry):
        cell = cells(o1_all, i)
        total = jnp.zeros((length, features), F32)
        for j in range(n):
            take = (cell == o2_all[j].astype(F32)).astype(BF16)
            total = total + nn(take, du2[j])
        dy1[i] = total.astype(BF16)
        skips[0:1, :] += jnp.sum(u1[i].astype(F32) * total, axis=0, keepdims=True)
        return carry

    lax.fori_loop(0, n, regrid_back, 0)
    clip_copies = []
    for d in range(1, clips):
        to = lax.rem(clip + d, clips)
        copy = copy_to("dp", to, skips, clips_in.at[clip], clip_send.at[d - 1], clip_recv.at[d - 1])
        copy.start()
        clip_copies.append(copy)
    clips_in[clip] = skips[...]

    def grads_first(i, carry):
        b = n - 1 - i
        dw, dr, dg, du, new = layer_grads(
            u1[b], dy1[b], w1_all[b], r1_all[b], Chunk(g1_all[b], size), skip1, states[b], adjoint[...], True
        )
        adjoint[...] = new
        du1[b] = du.astype(BF16)
        params1[b, 0] = dw.astype(BF16)
        params1[b, 1] = dr.astype(BF16)
        decays1[b] = dg

        @pl.when(b != me)
        def _():
            for copy in leave_first(b, lax.rem(b - me + n, n) - 1):
                copy.start()

        return carry

    lax.fori_loop(0, n, grads_first, 0)
    for copy in clip_copies:
        copy.wait()
    summed[...] = jnp.sum(clips_in[...], axis=0)
    last = []
    for d in range(1, n):
        to = lax.rem(me + d, n)
        copy = copy_to("seq", to, summed, parts_in.at[me], out_send.at[d - 1, 5], out_recv.at[d - 1, 5])
        copy.start()
        last.append(copy)
    parts_in[me] = summed[...]
    params1_in[me] = params1[me]
    params2_in[me] = params2[me]
    decays1_in[me] = decays1[me]
    decays2_in[me] = decays2[me]
    dinput[:, here] = du1[me]
    for group in arriving:
        for copy in group:
            copy.wait_send()
    for copy in far + near:
        copy.wait_send()
    for d in range(1, n):
        to = lax.rem(me + d, n)
        last += leave_second(to, d - 1) + leave_first(to, d - 1)
    for copy in last:
        copy.wait()


def whole(n, clips, size, u, w1, r1, g1, k1, w2, r2, g2, k2, o1, o2, ct):
    length, width = u.shape
    heads = g1.shape[1]
    count = w1.shape[1]
    features = heads * size
    vmem = pl.BlockSpec(memory_space=pltpu.VMEM)
    smem = pl.BlockSpec(memory_space=pltpu.SMEM)
    wide, param, params = (n, length, features), (n, length, count), (n, 2, length, count)
    decay, order, gain = (n, heads, length), (n, 1, length), (2, features)
    outs = (((length, width), BF16), (params, BF16), (params, BF16), (decay, F32), (decay, F32), ((n,) + gain, F32))
    held = [
        (wide, BF16),
        (param, BF16),
        (param, BF16),
        (decay, F32),
        (param, BF16),
        (param, BF16),
        (decay, F32),
        (order, jnp.int32),
        (order, jnp.int32),
        (wide, BF16),
        (wide, BF16),
        ((length, width), BF16),
        ((length, width), BF16),
        (wide, BF16),
        (wide, F32),
        (wide, BF16),
        (wide, BF16),
        (wide, BF16),
        ((n, features, count), F32),
        ((n, features, count), F32),
        ((features, count), F32),
        ((features, count), F32),
        (wide, BF16),
        (params, BF16),
        (params, BF16),
        (decay, F32),
        (decay, F32),
        (gain, F32),
        ((clips,) + gain, F32),
        (gain, F32),
    ]
    return pl.pallas_call(
        functools.partial(whole_kernel, n, clips, size),
        out_shape=tuple(jax.ShapeDtypeStruct(*out) for out in outs),
        in_specs=[vmem] * 4 + [smem] + [vmem] * 3 + [smem] + [vmem] * 3,
        out_specs=[vmem] * 6,
        scratch_shapes=[pltpu.VMEM(*one) for one in held]
        + [pltpu.SemaphoreType.DMA((n - 1, 7))] * 2
        + [pltpu.SemaphoreType.DMA((n - 1, 6))] * 2
        + [pltpu.SemaphoreType.DMA((clips - 1,))] * 2
        + [pltpu.SemaphoreType.DMA((n - 1, 4))] * 2,
        compiler_params=pltpu.CompilerParams(collective_id=0, has_side_effects=True),
        name="whole",
    )(u, w1, r1, g1, k1, w2, r2, g2, k2, o1, o2, ct)


def gather_kernel(n, factor, *refs):
    (du, params1, params2, decays1, decays2, parts) = refs[:6]
    (dinput, dw1, dr1, dg1, dk1, dw2, dr2, dg2, dk2) = refs[6:]
    heads = decays1.shape[1]
    width = parts.shape[2]
    size = width // heads
    dinput[...] = du[...]
    dg1[...] = decays1[...]
    dg2[...] = decays2[...]
    for params, outs in ((params1, (dw1, dr1)), (params2, (dw2, dr2))):
        for k, out in enumerate(outs):
            total = params[0, k].astype(F32)
            for s in range(1, n):
                total = total + params[s, k].astype(F32)
            out[...] = total.astype(BF16)
    picks = (iota((width, heads), 0) // size == iota((width, heads), 1)).astype(F32)
    for s in range(n):
        by_head = nn(parts[s], picks, HIGHEST) * factor
        dk1[:, s * heads : (s + 1) * heads] = by_head[0:1]
        dk2[:, s * heads : (s + 1) * heads] = by_head[1:2]


def gather(n, factor, du, params1, params2, decays1, decays2, parts):
    length, count = params1.shape[2:]
    heads = decays1.shape[1]
    vmem = pl.BlockSpec(memory_space=pltpu.VMEM)
    param = jax.ShapeDtypeStruct((length, count), BF16)
    decay = jax.ShapeDtypeStruct(decays1.shape, F32)
    skip = jax.ShapeDtypeStruct((1, n * heads), F32)
    layer = (param, param, decay, skip)
    return pl.pallas_call(
        functools.partial(gather_kernel, n, factor),
        out_shape=(jax.ShapeDtypeStruct(du.shape, BF16),) + layer + layer,
        in_specs=[vmem] * 6,
        out_specs=[vmem] * 9,
        name="gather",
    )(du, params1, params2, decays1, decays2, parts)


def on_device(n, clips, u, w1, r1, g1, k1, w2, r2, g2, k2, o1, o2, ct):
    length, features = u.shape[1:]
    head_count = k1.shape[0]
    size = features // head_count
    heads = head_count // n

    def by_device(g):
        return g.reshape(n, heads, length)

    results = whole(
        n,
        clips,
        size,
        u[0],
        w1[0],
        r1[0],
        by_device(g1),
        k1,
        w2[0],
        r2[0],
        by_device(g2),
        k2,
        o1[None],
        o2[None],
        ct[0],
    )
    factor = 1.0 / math.sqrt(clips * n * length * size)
    du, dw1, dr1, dg1, dk1, dw2, dr2, dg2, dk2 = gather(n, factor, *results)
    return (
        du[None],
        dw1[None],
        dr1[None],
        dg1.reshape(1, head_count, length),
        dk1[0],
        dw2[None],
        dr2[None],
        dg2.reshape(1, head_count, length),
        dk2[0],
    )


def solution(mesh):
    tokens, decay = P("dp", "seq", None), P("dp", None, "seq")
    return jax.shard_map(
        functools.partial(on_device, mesh.shape["seq"], mesh.shape["dp"]),
        mesh=mesh,
        in_specs=(tokens, tokens, tokens, decay, P(), tokens, tokens, decay, P(), P("seq"), P("seq"), tokens),
        out_specs=(tokens, tokens, tokens, decay, P(), tokens, tokens, decay, P()),
        check_vma=False,
    )
```
